32 devices in a mesh: clips: 2 (over x), tm: 4 (over y, core), height: 4 (over z).
Axes of the slice: x: 2, y: 2, z: 4, core: 2. Of those that a mesh axis runs over, the one named last changes fastest.
Arguments:
- features: bfloat16 [16, 16, 96, 512], P(('clips', 'tm'), 'height'), parts along dimension 0, may hold values from -1000 to 1000
- gain: float32 [512], replicated, may hold values from 0.1 to 1.9
- shift: float32 [512], replicated, may hold values from -3 to 3
- kernel: bfloat16 [3, 3, 3, 512, 256], replicated, may hold values from -0.0546875 to 0.0546875
- bias: float32 [256], replicated, may hold values from -3 to 3
Outputs:
- decoded: bfloat16 [16, 16, 96, 256], P(('clips', 'tm'), 'height'), parts along dimension 0
The draws below stay inside these ranges and needn't reach their ends.
There are 2 independent parts, one for each index of `clips`. The reference program is written for one: setup_inputs(seed, part) draws one part's arguments, and reference() takes and returns one part's arrays. A program takes and returns all parts, laid end to end along the dimension named above; an argument that names none is the same for every part. Nothing has to cross between parts.
All inputs are finite; a program needn't handle non-finite values.
Results may differ from the reference program's by a relative error of at most 0.0055.
Values may be sent and summed in bfloat16 or wider, within the bound.
No kernel may reach another device: no remote copies, remote signals or barrier semaphores. Data moves between devices by JAX's collectives and lax.ppermute only.
A program may use at most 64 MiB of HBM per device.

```python
import jax
import jax.numpy as jnp
from jax import lax

CHANNELS = 512
COUT = 256
GROUPS = 32
COLS = 96
FRAMES = 8
ROWS = 16


def draw_features(key, part):
    keys = jax.random.split(jax.random.fold_in(key, 17), 5)
    frame_pos = jnp.arange(FRAMES, dtype=jnp.float32) / max(FRAMES - 1, 1)
    frame_trend = jnp.exp(jnp.log(3.0) * frame_pos)
    chan_scale = jnp.exp(jax.random.uniform(keys[1], (CHANNELS,), jnp.float32, 0.0, jnp.log(10.0)))
    chan_offset = 0.5 * jax.random.normal(keys[2], (CHANNELS,), jnp.float32)
    noise = jnp.clip(jax.random.normal(keys[0], (FRAMES, ROWS, COLS, CHANNELS), jnp.float32), -6.0, 6.0)
    frame_random = jnp.exp(jax.random.uniform(keys[4], (FRAMES,), jnp.float32, -jnp.log(2.0), jnp.log(2.0)))
    frame_scale = frame_trend * frame_random
    values = (noise + chan_offset) * chan_scale
    values = values * frame_scale[:, None, None, None]
    values = jnp.clip(values, -1000.0, 1000.0)
    return values.astype(jnp.bfloat16)


def bell_draw(stream_key, extent, deviation, reach, held_as=jnp.bfloat16):
    result = deviation * jax.random.normal(stream_key, extent, jnp.float32)
    return jnp.clip(result, min=-reach, max=reach).astype(held_as)


def setup_inputs(seed: int = 0, part: int = 0) -> dict:
    key_list = jax.random.split(jax.random.key(seed), 6)
    part_splits = jax.random.split(jax.random.fold_in(key_list[5], part), 6)
    features = draw_features(jax.random.fold_in(jax.random.fold_in(key_list[5], part), 71), part)
    gain = jnp.clip(1.0 + 0.18 * jax.random.normal(key_list[1], (CHANNELS,), jnp.float32), 0.1, 1.9)
    shift = bell_draw(key_list[2], (CHANNELS,), 0.5, 3.0, jnp.float32)
    kernel = bell_draw(key_list[3], (3, 3, 3, CHANNELS, COUT), (27 * CHANNELS) ** -0.5, 0.0546875)
    bias = bell_draw(key_list[4], (COUT,), 0.5, 3.0, jnp.float32)
    return {"features": features, "gain": gain, "shift": shift, "kernel": kernel, "bias": bias}


epsilon = 1e-06

def reference(features, gain, shift, kernel, bias):
    per_group = CHANNELS // GROUPS
    wide_values = features.astype(jnp.float32).reshape(FRAMES, ROWS, COLS, GROUPS, per_group)
    cells_total = FRAMES * ROWS * COLS * per_group
    group_mean = lax.optimization_barrier(jnp.sum(wide_values, axis=(0, 1, 2, 4))) / cells_total
    centered = wide_values - group_mean[:, None]
    group_var = lax.optimization_barrier(jnp.sum(centered * centered, axis=(0, 1, 2, 4))) / cells_total
    normed = centered * lax.rsqrt(group_var + epsilon)[:, None]
    normed = normed.reshape(FRAMES, ROWS, COLS, CHANNELS) * gain + shift
    activated = jax.nn.silu(normed).astype(jnp.bfloat16)
    padded = jnp.concatenate([activated[:1], activated[:1], activated], 0)
    padded = jnp.pad(padded, ((0, 0), (1, 1), (1, 1), (0, 0)))

    def one_frame(position):
        slab = lax.dynamic_slice_in_dim(padded, position, 3, 0)
        summed = jnp.zeros((ROWS * COLS, COUT), jnp.float32)
        for a in range(3):
            for b in range(3):
                for c in range(3):
                    window = slab[a, b:b + ROWS, c:c + COLS, :].reshape(ROWS * COLS, CHANNELS)
                    summed = summed + jnp.dot(window, kernel[a, b, c], preferred_element_type=jnp.float32)
        return (summed.reshape(ROWS, COLS, COUT) + bias).astype(jnp.bfloat16)
    return lax.map(one_frame, jnp.arange(FRAMES, dtype=jnp.int32))
```

```python
import functools

import jax
import jax.numpy as jnp
from jax import lax
from jax.experimental import pallas as pl
from jax.experimental.pallas import tpu as pltpu
from jax.sharding import PartitionSpec as P

GROUPS = 32
LANES = 128
epsilon = 1e-06
both = ("tm", "height")


def stats_kernel(x_ref, out_ref):
    frames, rows, cols, channels = x_ref.shape
    tiles = channels // LANES
    total = jnp.zeros((8, channels), jnp.float32)
    squares = jnp.zeros((8, channels), jnp.float32)
    for f in range(frames):
        for r in range(rows):
            wide = x_ref[f, r].astype(jnp.float32).reshape(cols // 8, 8, channels)
            total = total + jnp.sum(wide, axis=0)
            squares = squares + jnp.sum(wide * wide, axis=0)
    total = jnp.sum(total, axis=0, keepdims=True)
    squares = jnp.sum(squares, axis=0, keepdims=True)
    for i in range(tiles):
        out_ref[i : i + 1, :] = total[:, i * LANES : (i + 1) * LANES]
        out_ref[tiles + i : tiles + i + 1, :] = squares[:, i * LANES : (i + 1) * LANES]


def local_stats(features):
    channels = features.shape[-1]
    return pl.pallas_call(
        stats_kernel,
        out_shape=jax.ShapeDtypeStruct((2 * channels // LANES, LANES), jnp.float32),
        name="stats",
    )(features)


def summed_over(value, axis):
    count = lax.axis_size(axis)
    if count & (count - 1):
        return lax.psum(value, axis)
    step = count // 2
    while step:
        value = value + lax.ppermute(value, axis, [(i, i ^ step) for i in range(count)])
        step //= 2
    return value


def moved(value, tm_step, height_step):
    tm, height = lax.axis_size("tm"), lax.axis_size("height")
    pairs = [
        (t * height + h, (t + tm_step) * height + h + height_step)
        for t in range(tm)
        for h in range(height)
        if 0 <= t + tm_step < tm and 0 <= h + height_step < height
    ]
    return lax.ppermute(value, both, pairs)


def conv_kernel(
    cells,
    sums_ref,
    gain_ref,
    shift_ref,
    bias_ref,
    own_ref,
    earlier_ref,
    above_ref,
    below_ref,
    early_above_ref,
    early_below_ref,
    kernel_ref,
    out_ref,
    raw,
    act,
    weights,
    acc,
    coef,
    slab_sem,
    weight_sem,
):
    frames, rows, cols, channels = own_ref.shape
    tiles = channels // LANES
    cout = out_ref.shape[-1]
    tm = lax.axis_index("tm")
    height = lax.axis_index("height")
    last = lax.axis_size("height") - 1

    def copies(first):
        early = [own_ref.at[0:1]] * 2 if first else [earlier_ref.at[0:1], earlier_ref.at[1:2]]
        early_above = [above_ref.at[0:1]] * 2 if first else [early_above_ref.at[0:1], early_above_ref.at[1:2]]
        early_below = [below_ref.at[0:1]] * 2 if first else [early_below_ref.at[0:1], early_below_ref.at[1:2]]
        n = 0
        out = []
        for i in range(2):
            for source, start, size in (
                (early[i], 1, rows),
                (early_above[i], 0, 1),
                (early_below[i], rows + 1, 1),
            ):
                out.append(
                    pltpu.make_async_copy(
                        source, raw.at[i : i + 1, start : start + size], slab_sem.at[3 + n]
                    )
                )
                n += 1
        return out

    own_copies = [
        pltpu.make_async_copy(own_ref, raw.at[2 : 2 + frames, 1 : 1 + rows], slab_sem.at[0]),
        pltpu.make_async_copy(above_ref, raw.at[2 : 2 + frames, 0:1], slab_sem.at[1]),
        pltpu.make_async_copy(below_ref, raw.at[2 : 2 + frames, rows + 1 : rows + 2], slab_sem.at[2]),
    ]
    for copy in own_copies:
        copy.start()

    @pl.when(tm == 0)
    def _():
        for copy in copies(True):
            copy.start()

    @pl.when(tm != 0)
    def _():
        for copy in copies(False):
            copy.start()

    weight_copies = [
        pltpu.make_async_copy(kernel_ref.at[a], weights.at[a], weight_sem.at[a]) for a in range(3)
    ]
    for copy in weight_copies:
        copy.start()

    per_group = channels // GROUPS
    row = lax.broadcasted_iota(jnp.int32, (LANES, LANES), 0) // per_group
    col = lax.broadcasted_iota(jnp.int32, (LANES, LANES), 1) // per_group
    same = jnp.where(row == col, 1.0, 0.0)
    grouped = jnp.dot(
        sums_ref[...], same, precision=lax.Precision.HIGHEST, preferred_element_type=jnp.float32
    )
    mean = grouped[:tiles] / cells
    var = grouped[tiles:] / cells - mean * mean
    scale = lax.rsqrt(var + epsilon) * gain_ref[...]
    offset = shift_ref[...] - mean * scale
    for i in range(tiles):
        coef[0:1, i * LANES : (i + 1) * LANES] = 0.5 * scale[i : i + 1]
        coef[1:2, i * LANES : (i + 1) * LANES] = 0.5 * offset[i : i + 1]

    for copy in own_copies:
        copy.wait()
    for copy in copies(False):
        copy.wait()

    half_scale = coef[0:1, :]
    half_offset = coef[1:2, :]
    top = jnp.where(height == 0, 0.0, 1.0)
    bottom = jnp.where(height == last, 0.0, 1.0)

    for f in range(2 + frames):
        for r in range(rows + 2):
            half = raw[f, r].astype(jnp.float32) * half_scale + half_offset
            value = half + half * jnp.tanh(half)
            if r == 0:
                value = value * top
            if r == rows + 1:
                value = value * bottom
            act[f, r] = value.astype(jnp.bfloat16)

    for copy in weight_copies:
        copy.wait()

    for c in range(3):
        total = None
        for a in range(3):
            windows = [
                act[a : a + frames, b : b + rows].reshape(frames * rows * cols, channels)
                for b in range(3)
            ]
            part = jnp.dot(
                jnp.concatenate(windows, axis=1),
                weights[a, :, c].reshape(3 * channels, cout),
                preferred_element_type=jnp.float32,
            )
            total = part if total is None else total + part
        acc[c] = total.reshape(frames * rows, cols, cout)

    place = lax.broadcasted_iota(jnp.int32, (cols, cout), 0)
    for i in range(frames * rows):
        left = jnp.where(place == 0, 0.0, pltpu.roll(acc[0, i], 1, 0))
        right = jnp.where(place == cols - 1, 0.0, pltpu.roll(acc[2, i], cols - 1, 0))
        out_ref[i // rows, i % rows] = (acc[1, i] + left + right + bias_ref[...]).astype(jnp.bfloat16)


def on_device(features, gain, shift, kernel, bias):
    frames, rows, cols, channels = features.shape
    cout = kernel.shape[-1]
    tiles = channels // LANES
    cells = lax.axis_size("tm") * lax.axis_size("height") * frames * rows * cols * (channels // GROUPS)
    first_row, last_row = features[:, :1], features[:, rows - 1 :]
    sums = local_stats(features)
    sums = summed_over(summed_over(sums, "tm"), "height")
    earlier = moved(features, 1, 0)
    above = moved(last_row, 0, 1)
    below = moved(first_row, 0, -1)
    early_above = moved(last_row, 1, 1)
    early_below = moved(first_row, 1, -1)
    vmem = pl.BlockSpec(memory_space=pltpu.VMEM)
    hbm = pl.BlockSpec(memory_space=pl.ANY)
    return pl.pallas_call(
        functools.partial(conv_kernel, float(cells)),
        out_shape=jax.ShapeDtypeStruct((frames, rows, cols, cout), jnp.bfloat16),
        in_specs=[vmem] * 4 + [hbm] * 7,
        out_specs=vmem,
        scratch_shapes=[
            pltpu.VMEM((2 + frames, rows + 2, cols, channels), jnp.bfloat16),
            pltpu.VMEM((2 + frames, rows + 2, cols, channels), jnp.bfloat16),
            pltpu.VMEM(kernel.shape, jnp.bfloat16),
            pltpu.VMEM((3, frames * rows, cols, cout), jnp.float32),
            pltpu.VMEM((8, channels), jnp.float32),
            pltpu.SemaphoreType.DMA((9,)),
            pltpu.SemaphoreType.DMA((3,)),
        ],
        compiler_params=pltpu.CompilerParams(vmem_limit_bytes=48 * 1024 * 1024),
        name="conv",
    )(
        sums,
        gain.reshape(tiles, LANES),
        shift.reshape(tiles, LANES),
        bias.reshape(1, cout),
        features,
        earlier,
        above,
        below,
        early_above,
        early_below,
        kernel,
    )


def solution(mesh):
    placed = (P(("clips", "tm"), "height", None, None), P(), P(), P(), P())
    return jax.shard_map(
        on_device,
        mesh=mesh,
        in_specs=placed,
        out_specs=P(("clips", "tm"), "height", None, None),
        check_vma=False,
    )
```

```python
import functools

import jax
import jax.numpy as jnp
from jax import lax
from jax.experimental import pallas as pl
from jax.experimental.pallas import tpu as pltpu
from jax.sharding import PartitionSpec as P


GROUPS = 32
LANES = 128
epsilon = 1e-06
both = ("tm", "height")


def stats_kernel(x_ref, sums_ref, edges_ref, held, sem):
    frames, rows, cols, channels = x_ref.shape
    tiles = channels // LANES
    copies = [
        pltpu.make_async_copy(x_ref.at[f, r], held.at[f, r], sem.at[f * rows + r])
        for f in range(frames)
        for r in range(rows)
    ]
    for copy in copies:
        copy.start()
    total = jnp.zeros((8, channels), jnp.float32)
    squares = jnp.zeros((8, channels), jnp.float32)
    for f in range(frames):
        for r in range(rows):
            copies[f * rows + r].wait()
            value = held[f, r]
            if r == 0:
                edges_ref[0, f, 0] = value
            if r == rows - 1:
                edges_ref[1, f, 0] = value
            wide = value.astype(jnp.float32).reshape(cols // 8, 8, channels)
            total = total + jnp.sum(wide, axis=0)
            squares = squares + jnp.sum(wide * wide, axis=0)
    total = jnp.sum(total, axis=0, keepdims=True)
    squares = jnp.sum(squares, axis=0, keepdims=True)
    for i in range(tiles):
        sums_ref[i : i + 1, :] = total[:, i * LANES : (i + 1) * LANES]
        sums_ref[tiles + i : tiles + i + 1, :] = squares[:, i * LANES : (i + 1) * LANES]


def local_stats(features):
    frames, rows, cols, channels = features.shape
    return pl.pallas_call(
        stats_kernel,
        out_shape=(
            jax.ShapeDtypeStruct((2 * channels // LANES, LANES), jnp.float32),
            jax.ShapeDtypeStruct((2, frames, 1, cols, channels), jnp.bfloat16),
        ),
        in_specs=[pl.BlockSpec(memory_space=pltpu.HBM)],
        scratch_shapes=[
            pltpu.VMEM(features.shape, jnp.bfloat16),
            pltpu.SemaphoreType.DMA((frames * rows,)),
        ],
        cost_estimate=pl.CostEstimate(flops=20_000_000_000, bytes_accessed=features.size * 2, transcendentals=0),
        compiler_params=pltpu.CompilerParams(vmem_limit_bytes=8 * 1024 * 1024),
        name="stats",
    )(features)


def summed_over(value, axis):
    count = lax.axis_size(axis)
    if count & (count - 1):
        return lax.psum(value, axis)
    step = count // 2
    while step:
        value = value + lax.ppermute(value, axis, [(i, i ^ step) for i in range(count)])
        step //= 2
    return value


def moved(value, tm_step, height_step):
    tm, height = lax.axis_size("tm"), lax.axis_size("height")
    pairs = [
        (t * height + h, (t + tm_step) * height + h + height_step)
        for t in range(tm)
        for h in range(height)
        if 0 <= t + tm_step < tm and 0 <= h + height_step < height
    ]
    return lax.ppermute(value, both, pairs)


def coefficients(cells, sums, gain, shift, coef):
    tiles = sums.shape[0] // 2
    per_group = tiles * LANES // GROUPS
    row = lax.broadcasted_iota(jnp.int32, (LANES, LANES), 0) // per_group
    col = lax.broadcasted_iota(jnp.int32, (LANES, LANES), 1) // per_group
    same = jnp.where(row == col, 1.0, 0.0)
    grouped = jnp.dot(
        sums, same, precision=lax.Precision.HIGHEST, preferred_element_type=jnp.float32
    )
    mean = grouped[:tiles] / cells
    var = grouped[tiles:] / cells - mean * mean
    scale = lax.rsqrt(var + epsilon) * gain
    offset = shift - mean * scale
    for i in range(tiles):
        coef[0:1, i * LANES : (i + 1) * LANES] = 0.5 * scale[i : i + 1]
        coef[1:2, i * LANES : (i + 1) * LANES] = 0.5 * offset[i : i + 1]


def activate(raw, act, coef, frames, rows):
    height = lax.axis_index("height")
    top = jnp.where(height == 0, 0.0, 1.0)
    bottom = jnp.where(height == lax.axis_size("height") - 1, 0.0, 1.0)
    half_scale = coef[0:1, :]
    half_offset = coef[1:2, :]
    for f in range(frames):
        for r in range(rows + 2):
            half = raw[f, r].astype(jnp.float32) * half_scale + half_offset
            value = half + half * jnp.tanh(half)
            if r == 0:
                value = value * top
            if r == rows + 1:
                value = value * bottom
            act[f, r] = value.astype(jnp.bfloat16)


def tap_sum(act, weights, slot, first, frames, rows, c):
    cols, channels = act.shape[2:]
    windows = [
        act[first : first + frames, b : b + rows].reshape(frames * rows * cols, channels)
        for b in range(3)
    ]
    return jnp.dot(
        jnp.concatenate(windows, axis=1),
        weights[slot, :, c].reshape(3 * channels, weights.shape[-1]),
        preferred_element_type=jnp.float32,
    )


def own_kernel(
    cells,
    sums_ref,
    gain_ref,
    shift_ref,
    bias_ref,
    own_ref,
    above_ref,
    below_ref,
    kernel_ref,
    out_ref,
    coef,
    raw,
    act,
    acc,
    sem,
):
    frames, rows, cols, _ = own_ref.shape
    cout = out_ref.shape[-1]
    slab = [
        pltpu.make_async_copy(own_ref, raw.at[:, 1 : 1 + rows], sem.at[0]),
        pltpu.make_async_copy(above_ref, raw.at[:, 0:1], sem.at[1]),
        pltpu.make_async_copy(below_ref, raw.at[:, rows + 1 : rows + 2], sem.at[2]),
    ]
    for copy in slab:
        copy.start()
    coefficients(cells, sums_ref[...], gain_ref[...], shift_ref[...], coef)
    for copy in slab:
        copy.wait()
    activate(raw, act, coef, frames, rows)

    for c in range(3):
        newest = tap_sum(act, kernel_ref, 2, 0, frames, rows, c)
        middle = tap_sum(act, kernel_ref, 1, 0, frames - 1, rows, c)
        whole = newest.reshape(frames, rows, cols, cout)
        acc[c, 0] = whole[0]
        acc[c, 1:] = whole[1:] + middle.reshape(frames - 1, rows, cols, cout)
    combine(acc, frames, rows, lambda f, r, value: store(out_ref, f, r, value + bias_ref[...]))


def store(ref, f, r, value):
    ref[f, r] = value.astype(ref.dtype)


def combine(acc, frames, rows, emit):
    cols, cout = acc.shape[3:]
    place = lax.broadcasted_iota(jnp.int32, (cols, cout), 0)
    for f in range(frames):
        for r in range(rows):
            left = jnp.where(place == 0, 0.0, pltpu.roll(acc[0, f, r], 1, 0))
            right = jnp.where(place == cols - 1, 0.0, pltpu.roll(acc[2, f, r], cols - 1, 0))
            emit(f, r, acc[1, f, r] + left + right)


def earlier_kernel(
    coef,
    partial_ref,
    own_ref,
    above_ref,
    below_ref,
    earlier_ref,
    early_above_ref,
    early_below_ref,
    kernel_ref,
    out_ref,
    raw,
    act,
    acc,
    sem,
):
    frames, rows, cols, _ = own_ref.shape
    cout = out_ref.shape[-1]
    tm = lax.axis_index("tm")

    def copies(first):
        out = []
        for i in range(2):
            source = 0 if first else frames - 2 + i
            for j, (ref, start, size) in enumerate(
                (
                    (own_ref if first else earlier_ref, 1, rows),
                    (above_ref if first else early_above_ref, 0, 1),
                    (below_ref if first else early_below_ref, rows + 1, 1),
                )
            ):
                out.append(
                    pltpu.make_async_copy(
                        ref.at[source], raw.at[i, start : start + size], sem.at[3 * i + j]
                    )
                )
        return out

    @pl.when(tm == 0)
    def _():
        for copy in copies(True):
            copy.start()

    @pl.when(tm != 0)
    def _():
        for copy in copies(False):
            copy.start()

    for copy in copies(False):
        copy.wait()
    activate(raw, act, coef, 2, rows)
    for c in range(3):
        oldest = tap_sum(act, kernel_ref, 0, 0, 2, rows, c).reshape(2, rows, cols, cout)
        middle = tap_sum(act, kernel_ref, 1, 1, 1, rows, c).reshape(1, rows, cols, cout)
        acc[c, 0] = oldest[0] + middle[0]
        acc[c, 1] = oldest[1]
    combine(acc, 2, rows, lambda f, r, value: store(out_ref, f, r, value + partial_ref[f, r]))
    for f in range(2, frames):
        for r in range(rows):
            out_ref[f, r] = partial_ref[f, r].astype(jnp.bfloat16)


def on_device(features, gain, shift, kernel, bias):
    frames, rows, cols, channels = features.shape
    cout = kernel.shape[-1]
    tiles = channels // LANES
    cells = lax.axis_size("tm") * lax.axis_size("height") * frames * rows * cols * (channels // GROUPS)
    vmem = pl.BlockSpec(memory_space=pltpu.VMEM)
    anywhere = pl.BlockSpec(memory_space=pl.ANY)
    params = pltpu.CompilerParams(vmem_limit_bytes=32 * 1024 * 1024)
    sums, edges = local_stats(features)
    sums = summed_over(summed_over(sums, "tm"), "height")
    above = moved(edges[1], 0, 1)
    below = moved(edges[0], 0, -1)
    earlier = moved(features, 1, 0)
    early_above = moved(edges[1], 1, 1)
    early_below = moved(edges[0], 1, -1)
    partial, coef = pl.pallas_call(
        functools.partial(own_kernel, float(cells)),
        out_shape=(
            jax.ShapeDtypeStruct((frames, rows, cols, cout), jnp.float32),
            jax.ShapeDtypeStruct((8, channels), jnp.float32),
        ),
        in_specs=[vmem] * 4 + [anywhere] * 3 + [vmem],
        out_specs=(vmem, vmem),
        scratch_shapes=[
            pltpu.VMEM((frames, rows + 2, cols, channels), jnp.bfloat16),
            pltpu.VMEM((frames, rows + 2, cols, channels), jnp.bfloat16),
            pltpu.VMEM((3, frames, rows, cols, cout), jnp.float32),
            pltpu.SemaphoreType.DMA((3,)),
        ],
        compiler_params=params,
        name="own",
    )(
        sums,
        gain.reshape(tiles, LANES),
        shift.reshape(tiles, LANES),
        bias.reshape(1, cout),
        features,
        above,
        below,
        kernel,
    )
    return pl.pallas_call(
        earlier_kernel,
        out_shape=jax.ShapeDtypeStruct((frames, rows, cols, cout), jnp.bfloat16),
        in_specs=[vmem, vmem] + [anywhere] * 6 + [vmem],
        out_specs=vmem,
        scratch_shapes=[
            pltpu.VMEM((2, rows + 2, cols, channels), jnp.bfloat16),
            pltpu.VMEM((2, rows + 2, cols, channels), jnp.bfloat16),
            pltpu.VMEM((3, 2, rows, cols, cout), jnp.float32),
            pltpu.SemaphoreType.DMA((6,)),
        ],
        compiler_params=params,
        name="earlier",
    )(coef, partial, features, above, below, earlier, early_above, early_below, kernel)


def solution(mesh):
    placed = (P(("clips", "tm"), "height", None, None), P(), P(), P(), P())
    tm, height = mesh.shape["tm"], mesh.shape["height"]
    for count in (tm, height):
        step = count // 2
        while step and not count & (count - 1):
            step //= 2
    step = jax.shard_map(
        on_device,
        mesh=mesh,
        in_specs=placed,
        out_specs=P(("clips", "tm"), "height", None, None),
        check_vma=False,
    )
    return step
```

```python
import functools

import jax
import jax.numpy as jnp
from jax import lax
from jax.experimental import pallas as pl
from jax.experimental.pallas import tpu as pltpu
from jax.sharding import PartitionSpec as P


GROUPS = 32
LANES = 128
epsilon = 1e-06


def stats_kernel(x_ref, sums_ref, edge_a_ref, edge_b_ref, held, sem):
    frames, rows, cols, channels = x_ref.shape
    tiles = channels // LANES
    copies = [
        pltpu.make_async_copy(x_ref.at[f, r], held.at[f, r], sem.at[f * rows + r])
        for f in range(frames)
        for r in range(rows)
    ]
    for copy in copies:
        copy.start()
    total = jnp.zeros((8, channels), jnp.float32)
    squares = jnp.zeros((8, channels), jnp.float32)
    for f in range(frames):
        for r in range(rows):
            copies[f * rows + r].wait()
            wide = held[f, r].astype(jnp.float32).reshape(cols // 8, 8, channels)
            total = total + jnp.sum(wide, axis=0)
            squares = squares + jnp.sum(wide * wide, axis=0)
    odd = lax.axis_index("height") % 2
    for f in range(frames):
        edge_a_ref[f] = held[f, (rows - 1) * (1 - odd)]
        edge_b_ref[f] = held[f, (rows - 1) * odd]
    total = jnp.sum(total, axis=0, keepdims=True)
    squares = jnp.sum(squares, axis=0, keepdims=True)
    for i in range(tiles):
        sums_ref[i : i + 1, :] = total[:, i * LANES : (i + 1) * LANES]
        sums_ref[tiles + i : tiles + i + 1, :] = squares[:, i * LANES : (i + 1) * LANES]


def local_stats(features):
    frames, rows, cols, channels = features.shape
    return pl.pallas_call(
        stats_kernel,
        out_shape=(
            jax.ShapeDtypeStruct((2 * channels // LANES, LANES), jnp.float32),
            jax.ShapeDtypeStruct((frames, cols, channels), jnp.bfloat16),
            jax.ShapeDtypeStruct((frames, cols, channels), jnp.bfloat16),
        ),
        in_specs=[pl.BlockSpec(memory_space=pltpu.HBM)],
        scratch_shapes=[
            pltpu.VMEM(features.shape, jnp.bfloat16),
            pltpu.SemaphoreType.DMA((frames * rows,)),
        ],
        cost_estimate=pl.CostEstimate(flops=20_000_000_000, bytes_accessed=features.size * 2, transcendentals=0),
        compiler_params=pltpu.CompilerParams(vmem_limit_bytes=8 * 1024 * 1024),
        name="stats",
    )(pltpu.with_memory_space_constraint(features, pltpu.HBM))


def summed_over(value, axis):
    count = lax.axis_size(axis)
    if count & (count - 1):
        return lax.psum(value, axis)
    step = count // 2
    while step:
        value = value + lax.ppermute(value, axis, [(i, i ^ step) for i in range(count)])
        step //= 2
    return value


def shifted(value):
    return lax.ppermute(value, "tm", [(i, i + 1) for i in range(lax.axis_size("tm") - 1)])


def swapped(value, start):
    pairs = [(i, i + 1) for i in range(start, lax.axis_size("height") - 1, 2)]
    return lax.ppermute(value, "height", pairs + [(j, i) for i, j in pairs])


def edge_slots(rows):
    odd = lax.axis_index("height") % 2
    return (rows + 1) * (1 - odd), (rows + 1) * odd


def coefficients(cells, sums, gain, shift, coef):
    tiles = sums.shape[0] // 2
    per_group = tiles * LANES // GROUPS
    row = lax.broadcasted_iota(jnp.int32, (LANES, LANES), 0) // per_group
    col = lax.broadcasted_iota(jnp.int32, (LANES, LANES), 1) // per_group
    same = jnp.where(row == col, 1.0, 0.0)
    grouped = jnp.dot(
        sums, same, precision=lax.Precision.HIGHEST, preferred_element_type=jnp.float32
    )
    mean = grouped[:tiles] / cells
    var = grouped[tiles:] / cells - mean * mean
    scale = lax.rsqrt(var + epsilon) * gain
    offset = shift - mean * scale
    for i in range(tiles):
        coef[0:1, i * LANES : (i + 1) * LANES] = 0.5 * scale[i : i + 1]
        coef[1:2, i * LANES : (i + 1) * LANES] = 0.5 * offset[i : i + 1]


def activate(raw, act, coef, frames, rows):
    height = lax.axis_index("height")
    top = jnp.where(height == 0, 0.0, 1.0)
    bottom = jnp.where(height == lax.axis_size("height") - 1, 0.0, 1.0)
    half_scale = coef[0:1, :]
    half_offset = coef[1:2, :]
    for f in range(frames):
        for r in range(rows + 2):
            half = raw[f, r].astype(jnp.float32) * half_scale + half_offset
            value = half + half * jnp.tanh(half)
            if r == 0:
                value = value * top
            if r == rows + 1:
                value = value * bottom
            act[f, r] = value.astype(jnp.bfloat16)


def tap_sum(act, weights, slot, first, frames, rows, c):
    cols, channels = act.shape[2:]
    windows = [
        act[first : first + frames, b : b + rows].reshape(frames * rows * cols, channels)
        for b in range(3)
    ]
    return jnp.dot(
        jnp.concatenate(windows, axis=1),
        weights[slot, :, c].reshape(3 * channels, weights.shape[-1]),
        preferred_element_type=jnp.float32,
    )


def own_kernel(
    cells,
    sums_ref,
    gain_ref,
    shift_ref,
    bias_ref,
    own_ref,
    edge_a_ref,
    edge_b_ref,
    kernel_ref,
    out_ref,
    coef,
    raw,
    act,
    acc,
    sem,
):
    frames, rows, cols, _ = own_ref.shape
    cout = out_ref.shape[-1]
    slot_a, slot_b = edge_slots(rows)
    slab = [
        pltpu.make_async_copy(own_ref, raw.at[:, 1 : 1 + rows], sem.at[0]),
        pltpu.make_async_copy(edge_a_ref, raw.at[:, slot_a], sem.at[1]),
        pltpu.make_async_copy(edge_b_ref, raw.at[:, slot_b], sem.at[2]),
    ]
    for copy in slab:
        copy.start()
    coefficients(cells, sums_ref[...], gain_ref[...], shift_ref[...], coef)
    for copy in slab:
        copy.wait()
    activate(raw, act, coef, frames, rows)

    for c in range(3):
        newest = tap_sum(act, kernel_ref, 2, 0, frames, rows, c)
        middle = tap_sum(act, kernel_ref, 1, 0, frames - 1, rows, c)
        whole = newest.reshape(frames, rows, cols, cout)
        acc[c, 0] = whole[0]
        acc[c, 1:] = whole[1:] + middle.reshape(frames - 1, rows, cols, cout)
    combine(acc, frames, rows, lambda f, r, value: store(out_ref, f, r, value + bias_ref[...]))


def store(ref, f, r, value):
    ref[f, r] = value.astype(ref.dtype)


def combine(acc, frames, rows, emit):
    cols, cout = acc.shape[3:]
    place = lax.broadcasted_iota(jnp.int32, (cols, cout), 0)
    for f in range(frames):
        for r in range(rows):
            left = jnp.where(place == 0, 0.0, pltpu.roll(acc[0, f, r], 1, 0))
            right = jnp.where(place == cols - 1, 0.0, pltpu.roll(acc[2, f, r], cols - 1, 0))
            emit(f, r, acc[1, f, r] + left + right)


def earlier_kernel(
    coef,
    partial_ref,
    own_ref,
    edge_a_ref,
    edge_b_ref,
    earlier_ref,
    corners_ref,
    kernel_ref,
    out_ref,
    raw,
    act,
    acc,
    sem,
):
    frames, rows, cols, _ = own_ref.shape
    cout = out_ref.shape[-1]
    tm = lax.axis_index("tm")

    slot_a, slot_b = edge_slots(rows)

    def copies(first):
        out = []
        for i in range(2):
            sources = (
                (own_ref.at[0], edge_a_ref.at[0], edge_b_ref.at[0])
                if first
                else (earlier_ref.at[i], corners_ref.at[i], corners_ref.at[2 + i])
            )
            targets = raw.at[i, 1 : 1 + rows], raw.at[i, slot_a], raw.at[i, slot_b]
            for j in range(3):
                out.append(pltpu.make_async_copy(sources[j], targets[j], sem.at[3 * i + j]))
        return out

    @pl.when(tm == 0)
    def _():
        for copy in copies(True):
            copy.start()

    @pl.when(tm != 0)
    def _():
        for copy in copies(False):
            copy.start()

    for copy in copies(False):
        copy.wait()
    activate(raw, act, coef, 2, rows)
    for c in range(3):
        oldest = tap_sum(act, kernel_ref, 0, 0, 2, rows, c).reshape(2, rows, cols, cout)
        middle = tap_sum(act, kernel_ref, 1, 1, 1, rows, c).reshape(1, rows, cols, cout)
        acc[c, 0] = oldest[0] + middle[0]
        acc[c, 1] = oldest[1]
    combine(acc, 2, rows, lambda f, r, value: store(out_ref, f, r, value + partial_ref[f, r]))
    for f in range(2, frames):
        for r in range(rows):
            out_ref[f, r] = partial_ref[f, r].astype(jnp.bfloat16)


def on_device(features, gain, shift, kernel, bias):
    frames, rows, cols, channels = features.shape
    cout = kernel.shape[-1]
    tiles = channels // LANES
    cells = lax.axis_size("tm") * lax.axis_size("height") * frames * rows * cols * (channels // GROUPS)
    vmem = pl.BlockSpec(memory_space=pltpu.VMEM)
    anywhere = pl.BlockSpec(memory_space=pl.ANY)
    params = pltpu.CompilerParams(vmem_limit_bytes=32 * 1024 * 1024)
    sums, edge_a, edge_b = local_stats(features)
    sums = summed_over(summed_over(sums, "tm"), "height")
    edge_a = swapped(edge_a, 0)
    edge_b = swapped(edge_b, 1)
    earlier = shifted(features[frames - 2 :])
    corners = shifted(jnp.concatenate([edge_a[frames - 2 :], edge_b[frames - 2 :]]))
    partial, coef = pl.pallas_call(
        functools.partial(own_kernel, float(cells)),
        out_shape=(
            jax.ShapeDtypeStruct((frames, rows, cols, cout), jnp.float32),
            jax.ShapeDtypeStruct((8, channels), jnp.float32),
        ),
        in_specs=[vmem] * 4 + [anywhere] * 3 + [vmem],
        out_specs=(vmem, vmem),
        scratch_shapes=[
            pltpu.VMEM((frames, rows + 2, cols, channels), jnp.bfloat16),
            pltpu.VMEM((frames, rows + 2, cols, channels), jnp.bfloat16),
            pltpu.VMEM((3, frames, rows, cols, cout), jnp.float32),
            pltpu.SemaphoreType.DMA((3,)),
        ],
        compiler_params=params,
        name="own",
    )(
        sums,
        gain.reshape(tiles, LANES),
        shift.reshape(tiles, LANES),
        bias.reshape(1, cout),
        features,
        edge_a,
        edge_b,
        kernel,
    )
    return pl.pallas_call(
        earlier_kernel,
        out_shape=jax.ShapeDtypeStruct((frames, rows, cols, cout), jnp.bfloat16),
        in_specs=[vmem, vmem] + [anywhere] * 5 + [vmem],
        out_specs=vmem,
        scratch_shapes=[
            pltpu.VMEM((2, rows + 2, cols, channels), jnp.bfloat16),
            pltpu.VMEM((2, rows + 2, cols, channels), jnp.bfloat16),
            pltpu.VMEM((3, 2, rows, cols, cout), jnp.float32),
            pltpu.SemaphoreType.DMA((6,)),
        ],
        compiler_params=params,
        name="earlier",
    )(coef, partial, features, edge_a, edge_b, earlier, corners, kernel)


def solution(mesh):
    placed = (P(("clips", "tm"), "height", None, None), P(), P(), P(), P())
    tm, height = mesh.shape["tm"], mesh.shape["height"]
    for count in (tm, height):
        step = count // 2
        while step and not count & (count - 1):
            step //= 2
    step = jax.shard_map(
        on_device,
        mesh=mesh,
        in_specs=placed,
        out_specs=P(("clips", "tm"), "height", None, None),
        check_vma=False,
    )
    return step
```

```python
import functools

import jax
import jax.numpy as jnp
from jax import lax
from jax.experimental import pallas as pl
from jax.experimental.pallas import tpu as pltpu
from jax.sharding import PartitionSpec as P


GROUPS = 32
LANES = 128
epsilon = 1e-06


def stats_kernel(x_ref, sums_ref, edge_a_ref, edge_b_ref, held, sem):
    frames, rows, cols, channels = x_ref.shape
    tiles = channels // LANES
    copies = [
        pltpu.make_async_copy(x_ref.at[f, r], held.at[f, r], sem.at[f * rows + r])
        for f in range(frames)
        for r in range(rows)
    ]
    for copy in copies:
        copy.start()
    total = jnp.zeros((8, channels), jnp.float32)
    squares = jnp.zeros((8, channels), jnp.float32)
    for f in range(frames):
        for r in range(rows):
            copies[f * rows + r].wait()
            wide = held[f, r].astype(jnp.float32).reshape(cols // 8, 8, channels)
            total = total + jnp.sum(wide, axis=0)
            squares = squares + jnp.sum(wide * wide, axis=0)
    odd = lax.axis_index("height") % 2
    for f in range(frames):
        edge_a_ref[f] = held[f, (rows - 1) * (1 - odd)]
        edge_b_ref[f] = held[f, (rows - 1) * odd]
    total = jnp.sum(total, axis=0, keepdims=True)
    squares = jnp.sum(squares, axis=0, keepdims=True)
    for i in range(tiles):
        sums_ref[i : i + 1, :] = total[:, i * LANES : (i + 1) * LANES]
        sums_ref[tiles + i : tiles + i + 1, :] = squares[:, i * LANES : (i + 1) * LANES]


def local_stats(features):
    frames, rows, cols, channels = features.shape
    return pl.pallas_call(
        stats_kernel,
        out_shape=(
            jax.ShapeDtypeStruct((2 * channels // LANES, LANES), jnp.float32),
            jax.ShapeDtypeStruct((frames, cols, channels), jnp.bfloat16),
            jax.ShapeDtypeStruct((frames, cols, channels), jnp.bfloat16),
        ),
        in_specs=[pl.BlockSpec(memory_space=pltpu.HBM)],
        scratch_shapes=[
            pltpu.VMEM(features.shape, jnp.bfloat16),
            pltpu.SemaphoreType.DMA((frames * rows,)),
        ],
        cost_estimate=pl.CostEstimate(flops=20_000_000_000, bytes_accessed=features.size * 2, transcendentals=0),
        compiler_params=pltpu.CompilerParams(vmem_limit_bytes=8 * 1024 * 1024),
        name="stats",
    )(pltpu.with_memory_space_constraint(features, pltpu.HBM))


def summed_over(value, axis):
    count = lax.axis_size(axis)
    if count & (count - 1):
        return lax.psum(value, axis)
    step = count // 2
    while step:
        value = value + lax.ppermute(value, axis, [(i, i ^ step) for i in range(count)])
        step //= 2
    return value


def shifted(value):
    return lax.ppermute(value, "tm", [(i, i + 1) for i in range(lax.axis_size("tm") - 1)])


def swapped(value, start):
    pairs = [(i, i + 1) for i in range(start, lax.axis_size("height") - 1, 2)]
    return lax.ppermute(value, "height", pairs + [(j, i) for i, j in pairs])


def coefficients(cells, sums, gain, shift, coef):
    tiles = sums.shape[0] // 2
    per_group = tiles * LANES // GROUPS
    row = lax.broadcasted_iota(jnp.int32, (LANES, LANES), 0) // per_group
    col = lax.broadcasted_iota(jnp.int32, (LANES, LANES), 1) // per_group
    same = jnp.where(row == col, 1.0, 0.0)
    grouped = jnp.dot(
        sums, same, precision=lax.Precision.HIGHEST, preferred_element_type=jnp.float32
    )
    mean = grouped[:tiles] / cells
    var = grouped[tiles:] / cells - mean * mean
    scale = lax.rsqrt(var + epsilon) * gain
    offset = shift - mean * scale
    for i in range(tiles):
        coef[0:1, i * LANES : (i + 1) * LANES] = 0.5 * scale[i : i + 1]
        coef[1:2, i * LANES : (i + 1) * LANES] = 0.5 * offset[i : i + 1]


def activate(source, act, coef, edge, rows):
    half_scale = coef[0:1, :]
    half_offset = coef[1:2, :]
    for r in range(rows + 2):
        half = source(r).astype(jnp.float32) * half_scale + half_offset
        value = half + half * jnp.tanh(half)
        if r == 0:
            value = value * edge[0]
        if r == rows + 1:
            value = value * edge[1]
        act[r] = value.astype(jnp.bfloat16)


def edge_masks():
    height = lax.axis_index("height")
    return (
        jnp.where(height == 0, 0.0, 1.0),
        jnp.where(height == lax.axis_size("height") - 1, 0.0, 1.0),
    )


def tap_sum(slabs, kernel_ref, first, rows, emit):
    cols, channels = slabs[0].shape[1:]
    cout = kernel_ref.shape[-1]
    taps = slice(first, first + len(slabs))

    def product(c):
        windows = [
            slab[b : b + rows].reshape(rows * cols, channels) for slab in slabs for b in range(3)
        ]
        return jnp.dot(
            jnp.concatenate(windows, axis=1),
            kernel_ref[taps, :, c].reshape(len(slabs) * 3 * channels, cout),
            preferred_element_type=jnp.float32,
        ).reshape(rows, cols, cout)

    left, right, middle = product(0), product(2), product(1)
    place = lax.broadcasted_iota(jnp.int32, (cols, cout), 0)
    for r in range(rows):
        from_left = jnp.where(place == 0, 0.0, pltpu.roll(left[r], 1, 0))
        from_right = jnp.where(place == cols - 1, 0.0, pltpu.roll(right[r], cols - 1, 0))
        emit(r, middle[r] + from_left + from_right)


def own_kernel(
    cells,
    sums_ref,
    gain_ref,
    shift_ref,
    bias_ref,
    own_ref,
    edge_a_ref,
    edge_b_ref,
    kernel_ref,
    out_ref,
    coef,
    *acts,
):
    frames, rows = own_ref.shape[:2]
    odd = lax.axis_index("height") % 2 == 1
    edge = edge_masks()
    coefficients(cells, sums_ref[...], gain_ref[...], shift_ref[...], coef)

    def source(f):
        def row(r):
            if r == 0:
                return jnp.where(odd, edge_a_ref[f], edge_b_ref[f])
            if r == rows + 1:
                return jnp.where(odd, edge_b_ref[f], edge_a_ref[f])
            return own_ref[f, r - 1]

        return row

    for f in range(frames):
        activate(source(f), acts[f], coef, edge, rows)

        def emit(r, value, f=f):
            out_ref[f, r] = value + bias_ref[...]

        tap_sum(acts[max(0, f - 2) : f + 1], kernel_ref, max(0, 2 - f), rows, emit)


def earlier_kernel(
    coef,
    partial_ref,
    own_ref,
    edge_a_ref,
    edge_b_ref,
    earlier_ref,
    corners_ref,
    kernel_ref,
    out_ref,
    old_act,
    new_act,
    staged,
    sem,
):
    frames, rows = own_ref.shape[:2]
    odd = lax.axis_index("height") % 2 == 1
    start = lax.axis_index("tm") == 0
    edge = edge_masks()

    def source(i):
        def row(r):
            if 0 < r <= rows:
                return jnp.where(start, own_ref[0, r - 1], earlier_ref[i, r - 1])
            a = jnp.where(start, edge_a_ref[0], corners_ref[i])
            b = jnp.where(start, edge_b_ref[0], corners_ref[2 + i])
            return jnp.where(odd, a, b) if r == 0 else jnp.where(odd, b, a)

        return row

    copies = []

    def finish(f, slabs, first):
        if slabs:

            def emit(r, value):
                staged[f, r] = (value + partial_ref[f, r]).astype(jnp.bfloat16)

            tap_sum(slabs, kernel_ref, first, rows, emit)
        else:
            for r in range(rows):
                staged[f, r] = partial_ref[f, r].astype(jnp.bfloat16)
        copy = pltpu.make_async_copy(staged.at[f], out_ref.at[f], sem.at[f])
        copy.start()
        copies.append(copy)

    for f in range(2, frames):
        finish(f, (), 0)
    activate(source(1), new_act, coef, edge, rows)
    finish(1, (new_act,), 0)
    activate(source(0), old_act, coef, edge, rows)
    finish(0, (old_act, new_act), 0)
    for copy in copies:
        copy.wait()


def on_device(features, gain, shift, kernel, bias):
    frames, rows, cols, channels = features.shape
    cout = kernel.shape[-1]
    tiles = channels // LANES
    cells = lax.axis_size("tm") * lax.axis_size("height") * frames * rows * cols * (channels // GROUPS)
    vmem = pl.BlockSpec(memory_space=pltpu.VMEM)
    params = pltpu.CompilerParams(vmem_limit_bytes=32 * 1024 * 1024)
    sums, edge_a, edge_b = local_stats(features)
    sums = summed_over(summed_over(sums, "tm"), "height")
    edge_a = swapped(edge_a, 0)
    edge_b = swapped(edge_b, 1)
    earlier = shifted(features[frames - 2 :])
    corners = shifted(jnp.concatenate([edge_a[frames - 2 :], edge_b[frames - 2 :]]))
    partial, coef = pl.pallas_call(
        functools.partial(own_kernel, float(cells)),
        out_shape=(
            jax.ShapeDtypeStruct((frames, rows, cols, cout), jnp.float32),
            jax.ShapeDtypeStruct((8, channels), jnp.float32),
        ),
        in_specs=[vmem] * 8,
        out_specs=(vmem, vmem),
        scratch_shapes=[pltpu.VMEM((rows + 2, cols, channels), jnp.bfloat16)] * frames,
        compiler_params=params,
        name="own",
    )(
        sums,
        gain.reshape(tiles, LANES),
        shift.reshape(tiles, LANES),
        bias.reshape(1, cout),
        features,
        edge_a,
        edge_b,
        kernel,
    )
    return pl.pallas_call(
        earlier_kernel,
        out_shape=jax.ShapeDtypeStruct((frames, rows, cols, cout), jnp.bfloat16),
        in_specs=[vmem] * 8,
        out_specs=pl.BlockSpec(memory_space=pltpu.HBM),
        scratch_shapes=[
            pltpu.VMEM((rows + 2, cols, channels), jnp.bfloat16),
            pltpu.VMEM((rows + 2, cols, channels), jnp.bfloat16),
            pltpu.VMEM((frames, rows, cols, cout), jnp.bfloat16),
            pltpu.SemaphoreType.DMA((frames,)),
        ],
        compiler_params=params,
        name="earlier",
    )(coef, partial, features, edge_a, edge_b, earlier, corners, kernel)


def solution(mesh):
    placed = (P(("clips", "tm"), "height", None, None), P(), P(), P(), P())
    tm, height = mesh.shape["tm"], mesh.shape["height"]
    for count in (tm, height):
        step = count // 2
        while step and not count & (count - 1):
            step //= 2
    step = jax.shard_map(
        on_device,
        mesh=mesh,
        in_specs=placed,
        out_specs=P(("clips", "tm"), "height", None, None),
        check_vma=False,
    )
    return step
```

```python
import functools

import jax
import jax.numpy as jnp
from jax import lax
from jax.experimental import pallas as pl
from jax.experimental.pallas import tpu as pltpu
from jax.sharding import PartitionSpec as P


GROUPS = 32
LANES = 128
epsilon = 1e-06


def stats_kernel(x_ref, sums_ref, edge_a_ref, edge_b_ref, held, sem):
    frames, rows, cols, channels = x_ref.shape
    tiles = channels // LANES
    copies = [
        pltpu.make_async_copy(x_ref.at[f, r], held.at[f, r], sem.at[f * rows + r])
        for f in range(frames)
        for r in range(rows)
    ]
    for copy in copies:
        copy.start()
    total = jnp.zeros((8, channels), jnp.float32)
    squares = jnp.zeros((8, channels), jnp.float32)
    for f in range(frames):
        for r in range(rows):
            copies[f * rows + r].wait()
            wide = held[f, r].astype(jnp.float32).reshape(cols // 8, 8, channels)
            total = total + jnp.sum(wide, axis=0)
            squares = squares + jnp.sum(wide * wide, axis=0)
    odd = lax.axis_index("height") % 2
    for f in range(frames):
        edge_a_ref[f] = held[f, (rows - 1) * (1 - odd)]
        edge_b_ref[f] = held[f, (rows - 1) * odd]
    total = jnp.sum(total, axis=0, keepdims=True)
    squares = jnp.sum(squares, axis=0, keepdims=True)
    for i in range(tiles):
        sums_ref[i : i + 1, :] = total[:, i * LANES : (i + 1) * LANES]
        sums_ref[tiles + i : tiles + i + 1, :] = squares[:, i * LANES : (i + 1) * LANES]


def local_stats(features):
    frames, rows, cols, channels = features.shape
    return pl.pallas_call(
        stats_kernel,
        out_shape=(
            jax.ShapeDtypeStruct((2 * channels // LANES, LANES), jnp.float32),
            jax.ShapeDtypeStruct((frames, cols, channels), jnp.bfloat16),
            jax.ShapeDtypeStruct((frames, cols, channels), jnp.bfloat16),
        ),
        in_specs=[pl.BlockSpec(memory_space=pltpu.HBM)],
        scratch_shapes=[
            pltpu.VMEM(features.shape, jnp.bfloat16),
            pltpu.SemaphoreType.DMA((frames * rows,)),
        ],
        cost_estimate=pl.CostEstimate(flops=20_000_000_000, bytes_accessed=features.size * 2, transcendentals=0),
        compiler_params=pltpu.CompilerParams(vmem_limit_bytes=8 * 1024 * 1024),
        name="stats",
    )(pltpu.with_memory_space_constraint(features, pltpu.HBM))


def round_steps(count):
    steps = [1 << i for i in range(count.bit_length() - 1)]
    return steps


def summed_over(value, axis):
    count = lax.axis_size(axis)
    if count & (count - 1):
        return lax.psum(value, axis)
    for step in round_steps(count):
        value = value + lax.ppermute(value, axis, [(i, i ^ step) for i in range(count)])
    return value


def shifted(value):
    return lax.ppermute(value, "tm", [(i, i + 1) for i in range(lax.axis_size("tm") - 1)])


def swapped(value, start):
    pairs = [(i, i + 1) for i in range(start, lax.axis_size("height") - 1, 2)]
    return lax.ppermute(value, "height", pairs + [(j, i) for i, j in pairs])


def coefficients(cells, sums, gain, shift, coef):
    tiles = sums.shape[0] // 2
    per_group = tiles * LANES // GROUPS
    row = lax.broadcasted_iota(jnp.int32, (LANES, LANES), 0) // per_group
    col = lax.broadcasted_iota(jnp.int32, (LANES, LANES), 1) // per_group
    same = jnp.where(row == col, 1.0, 0.0)
    grouped = jnp.dot(
        sums, same, precision=lax.Precision.HIGHEST, preferred_element_type=jnp.float32
    )
    mean = grouped[:tiles] / cells
    var = grouped[tiles:] / cells - mean * mean
    scale = lax.rsqrt(var + epsilon) * gain
    offset = shift - mean * scale
    for i in range(tiles):
        coef[0:1, i * LANES : (i + 1) * LANES] = 0.5 * scale[i : i + 1]
        coef[1:2, i * LANES : (i + 1) * LANES] = 0.5 * offset[i : i + 1]


def activate(source, act, coef, edge, rows):
    half_scale = coef[0:1, :]
    half_offset = coef[1:2, :]
    for r in range(rows + 2):
        half = source(r).astype(jnp.float32) * half_scale + half_offset
        value = half + half * jnp.tanh(half)
        if r == 0:
            value = value * edge[0]
        if r == rows + 1:
            value = value * edge[1]
        act[r] = value.astype(jnp.bfloat16)


def edge_masks():
    height = lax.axis_index("height")
    return (
        jnp.where(height == 0, 0.0, 1.0),
        jnp.where(height == lax.axis_size("height") - 1, 0.0, 1.0),
    )


def tap_sum(slabs, kernel_ref, first, rows, emit):
    cols, channels = slabs[0].shape[1:]
    cout = kernel_ref.shape[-1]
    taps = slice(first, first + len(slabs))

    def product(c):
        windows = [
            slab[b : b + rows].reshape(rows * cols, channels) for slab in slabs for b in range(3)
        ]
        return jnp.dot(
            jnp.concatenate(windows, axis=1),
            kernel_ref[taps, :, c].reshape(len(slabs) * 3 * channels, cout),
            preferred_element_type=jnp.float32,
        ).reshape(rows, cols, cout)

    left, right, middle = product(0), product(2), product(1)
    place = lax.broadcasted_iota(jnp.int32, (cols, cout), 0)
    for r in range(rows):
        from_left = jnp.where(place == 0, 0.0, pltpu.roll(left[r], 1, 0))
        from_right = jnp.where(place == cols - 1, 0.0, pltpu.roll(right[r], cols - 1, 0))
        emit(r, middle[r] + from_left + from_right)


def own_kernel(
    cells,
    sums_ref,
    gain_ref,
    shift_ref,
    bias_ref,
    own_ref,
    edge_a_ref,
    edge_b_ref,
    kernel_ref,
    out_ref,
    coef,
    *acts,
):
    frames, rows = own_ref.shape[:2]
    odd = lax.axis_index("height") % 2 == 1
    edge = edge_masks()
    coefficients(cells, sums_ref[...], gain_ref[...], shift_ref[...], coef)

    def source(f):
        def row(r):
            if r == 0:
                return jnp.where(odd, edge_a_ref[f], edge_b_ref[f])
            if r == rows + 1:
                return jnp.where(odd, edge_b_ref[f], edge_a_ref[f])
            return own_ref[f, r - 1]

        return row

    for f in range(frames):
        activate(source(f), acts[f], coef, edge, rows)

        def emit(r, value, f=f):
            out_ref[f, r] = value + bias_ref[...]

        tap_sum(acts[max(0, f - 2) : f + 1], kernel_ref, max(0, 2 - f), rows, emit)


def earlier_kernel(
    coef,
    partial_ref,
    own_ref,
    edge_a_ref,
    edge_b_ref,
    earlier_ref,
    corners_ref,
    kernel_ref,
    out_ref,
    old_act,
    new_act,
    staged,
    sem,
):
    frames, rows = own_ref.shape[:2]
    odd = lax.axis_index("height") % 2 == 1
    start = lax.axis_index("tm") == 0
    edge = edge_masks()

    def source(i):
        def row(r):
            if 0 < r <= rows:
                return jnp.where(start, own_ref[0, r - 1], earlier_ref[i, r - 1])
            a = jnp.where(start, edge_a_ref[0], corners_ref[i])
            b = jnp.where(start, edge_b_ref[0], corners_ref[2 + i])
            return jnp.where(odd, a, b) if r == 0 else jnp.where(odd, b, a)

        return row

    copies = []

    def finish(f, slabs, first):
        if slabs:

            def emit(r, value):
                staged[f, r] = (value + partial_ref[f, r]).astype(jnp.bfloat16)

            tap_sum(slabs, kernel_ref, first, rows, emit)
        else:
            for r in range(rows):
                staged[f, r] = partial_ref[f, r].astype(jnp.bfloat16)
        copy = pltpu.make_async_copy(staged.at[f], out_ref.at[f], sem.at[f])
        copy.start()
        copies.append(copy)

    for f in range(2, frames):
        finish(f, (), 0)
    activate(source(1), new_act, coef, edge, rows)
    finish(1, (new_act,), 0)
    activate(source(0), old_act, coef, edge, rows)
    finish(0, (old_act, new_act), 0)
    for copy in copies:
        copy.wait()


def on_device(features, gain, shift, kernel, bias):
    frames, rows, cols, channels = features.shape
    cout = kernel.shape[-1]
    tiles = channels // LANES
    cells = lax.axis_size("tm") * lax.axis_size("height") * frames * rows * cols * (channels // GROUPS)
    vmem = pl.BlockSpec(memory_space=pltpu.VMEM)
    params = pltpu.CompilerParams(vmem_limit_bytes=32 * 1024 * 1024)
    sums, edge_a, edge_b = local_stats(features)
    sums = summed_over(summed_over(sums, "tm"), "height")
    edge_a = swapped(edge_a, 0)
    edge_b = swapped(edge_b, 1)
    earlier = shifted(features[frames - 2 :])
    corners = shifted(jnp.concatenate([edge_a[frames - 2 :], edge_b[frames - 2 :]]))
    partial, coef = pl.pallas_call(
        functools.partial(own_kernel, float(cells)),
        out_shape=(
            jax.ShapeDtypeStruct((frames, rows, cols, cout), jnp.float32),
            jax.ShapeDtypeStruct((8, channels), jnp.float32),
        ),
        in_specs=[vmem] * 8,
        out_specs=(vmem, vmem),
        scratch_shapes=[pltpu.VMEM((rows + 2, cols, channels), jnp.bfloat16)] * frames,
        compiler_params=params,
        name="own",
    )(
        sums,
        gain.reshape(tiles, LANES),
        shift.reshape(tiles, LANES),
        bias.reshape(1, cout),
        features,
        edge_a,
        edge_b,
        kernel,
    )
    return pl.pallas_call(
        earlier_kernel,
        out_shape=jax.ShapeDtypeStruct((frames, rows, cols, cout), jnp.bfloat16),
        in_specs=[vmem] * 8,
        out_specs=pl.BlockSpec(memory_space=pltpu.HBM),
        scratch_shapes=[
            pltpu.VMEM((rows + 2, cols, channels), jnp.bfloat16),
            pltpu.VMEM((rows + 2, cols, channels), jnp.bfloat16),
            pltpu.VMEM((frames, rows, cols, cout), jnp.bfloat16),
            pltpu.SemaphoreType.DMA((frames,)),
        ],
        compiler_params=params,
        name="earlier",
    )(coef, partial, features, edge_a, edge_b, earlier, corners, kernel)


def solution(mesh):
    placed = (P(("clips", "tm"), "height", None, None), P(), P(), P(), P())
    return jax.shard_map(
        on_device,
        mesh=mesh,
        in_specs=placed,
        out_specs=P(("clips", "tm"), "height", None, None),
        check_vma=False,
    )
```
